32 devices in a mesh: cat: 2 (over x), lat: 4 (over y, core), lon: 4 (over z).
Axes of the slice: x: 2, y: 2, z: 4, core: 2. Of those that a mesh axis runs over, the one named last changes fastest.
Arguments:
- thickness: bfloat16 [40, 1024, 2560], P('cat', 'lat', 'lon'), may hold values from 0.099609375 to 4
- area: bfloat16 [40, 1024, 2560], P('cat', 'lat', 'lon'), may hold values from 0.0049743652 to 0.049804688
- ridge_weight: float32 [40], P('cat'), may hold values from 0.2 to 2
- cat_top: int32 [1024, 2560], P('lat', 'lon'), may hold values from 1 to 40
- land_mask: int32 [1024, 2560], P('lat', 'lon'), may hold values 0 or 1
- velocity_u: float32 [1024, 2560], P('lat', 'lon'), may hold values from -1.8 to 1.8
- velocity_v: float32 [1024, 2560], P('lat', 'lon'), may hold values from -1.8 to 1.8
- stress_div: float32 [1024, 2560], P('lat', 'lon'), may hold values from -3 to 3
- stress_ten: float32 [1024, 2560], P('lat', 'lon'), may hold values from -3 to 3
- stress_shear: float32 [1024, 2560], P('lat', 'lon'), may hold values from -3 to 3
- wind_x: float32 [1024, 2560], P('lat', 'lon'), may hold values from -6 to 6
- wind_y: float32 [1024, 2560], P('lat', 'lon'), may hold values from -6 to 6
- water_drag: float32 [1024, 2560], P('lat', 'lon'), may hold values from 0.2 to 2
Outputs:
- new_u: float32 [1024, 2560], P('lat', 'lon')
- new_v: float32 [1024, 2560], P('lat', 'lon')
- new_div: float32 [1024, 2560], P('lat', 'lon')
- new_ten: float32 [1024, 2560], P('lat', 'lon')
- new_shear: float32 [1024, 2560], P('lat', 'lon')
The draws below stay inside these ranges and needn't reach their ends.
Inputs may be any that keep to these rules, and one draw needn't show every extreme that they name: Categories with index cat_top or above are absent from a cell.
All inputs are finite; a program needn't handle non-finite values. No bound on the sum of `land_mask` on one device may be relied on, other than what follows from the above.
Results may differ from the reference program's by a relative error of at most 0.0003.
Values sent between devices are 32-bit elements; how exact they have to be, the bound alone decides.
A program may use at most 128 MiB of HBM per device.

```python
import math
import jax
import jax.numpy as jnp
from jax import lax

NCAT = 40
SUB = 4
NLAT = 1024
NLON = 2560


def with_ends(entries, stream_key, least, high):
    shape = entries.shape
    spot = [jax.random.randint(jax.random.fold_in(stream_key, axis), (), 0, shape[axis]) for axis in range(len(shape))]
    entries = entries.at[tuple(spot)].set(least)
    longest = shape.index(max(shape))
    spot[longest] = (spot[longest] + 1) % shape[longest]
    return entries.at[tuple(spot)].set(high)


def shard_levels(rng, extent, cuts, low, high):
    factor_of = 1.0
    for axis_at, shards_of in cuts:
        steps = jax.random.uniform(jax.random.fold_in(jax.random.fold_in(rng, 6), axis_at), (shards_of,), jnp.float32, low / len(cuts), high / len(cuts))
        factor_of = factor_of * jnp.repeat(jnp.exp(steps), extent[axis_at] // shards_of).reshape((-1,) + (1,) * (len(extent) - 1 - axis_at))
    return factor_of


def noise(own_key, shape, deviation, limit, cuts=(), dtype=jnp.bfloat16):
    drawn = jax.random.normal(own_key, shape, jnp.float32) * deviation
    if len(cuts) > 0:
        drawn = shard_levels(own_key, shape, cuts, -0.22, 0.18) * drawn
    return jnp.clip(drawn, min=-limit, max=limit).astype(dtype)


def setup_inputs(seed: int = 0) -> dict:
    streams_of = jax.random.split(jax.random.key(seed), 14)
    return {
        "thickness": jnp.clip(jnp.exp(math.log(4.0) - 3.6927934 * jax.random.uniform(streams_of[0], (NCAT, NLAT, NLON), jnp.float32) ** shard_levels(streams_of[0], (NCAT, NLAT, NLON), ((0, 2), (1, 4), (2, 4)), -0.2, 0.2)), 0.099609375, 4.0).astype(jnp.bfloat16),
        "area": jnp.clip(jnp.exp(math.log(0.049804688) - 2.3038113 * jax.random.uniform(streams_of[1], (NCAT, NLAT, NLON), jnp.float32) ** shard_levels(streams_of[1], (NCAT, NLAT, NLON), ((0, 2), (1, 4), (2, 4)), -0.2, 0.2)), 0.0049743652, 0.049804688).astype(jnp.bfloat16),
        "ridge_weight": jnp.clip(jnp.exp(math.log(2.0) - 2.3025851 * jax.random.uniform(streams_of[2], (NCAT,), jnp.float32) ** shard_levels(streams_of[2], (NCAT,), ((0, 2),), -0.2, 0.2)), 0.2, 2.0),
        "cat_top": with_ends(jax.random.randint(streams_of[3], (NLAT, NLON), 1, NCAT + 1), jax.random.fold_in(streams_of[3], 1), 1, NCAT).astype(jnp.int32),
        "land_mask": with_ends((jax.random.randint(streams_of[4], (NLAT, NLON), 0, 10) < 9).astype(jnp.int32), jax.random.fold_in(streams_of[4], 1), 0, 1),
        "velocity_u": noise(streams_of[5], (NLAT, NLON), 0.3, 1.8, ((0, 4), (1, 4)), jnp.float32),
        "velocity_v": noise(streams_of[6], (NLAT, NLON), 0.3, 1.8, ((0, 4), (1, 4)), jnp.float32),
        "stress_div": noise(streams_of[7], (NLAT, NLON), 0.5, 3.0, ((0, 4), (1, 4)), jnp.float32),
        "stress_ten": noise(streams_of[8], (NLAT, NLON), 0.5, 3.0, ((0, 4), (1, 4)), jnp.float32),
        "stress_shear": noise(streams_of[9], (NLAT, NLON), 0.5, 3.0, ((0, 4), (1, 4)), jnp.float32),
        "wind_x": noise(streams_of[10], (NLAT, NLON), 1.0, 6.0, ((0, 4), (1, 4)), jnp.float32),
        "wind_y": noise(streams_of[11], (NLAT, NLON), 1.0, 6.0, ((0, 4), (1, 4)), jnp.float32),
        "water_drag": jnp.clip(jnp.exp(math.log(2.0) - 2.3025851 * jax.random.uniform(streams_of[12], (NLAT, NLON), jnp.float32) ** shard_levels(streams_of[12], (NLAT, NLON), ((0, 4), (1, 4)), -0.2, 0.2)), 0.2, 2.0),
    }


ELASTIC = 2.0
ECC_SQUARED = 4.0
DELTA_FLOOR = 0.05
CORIOLIS = 0.5

def slopes(along, across):
    return (0.5 * (along[:, :, 2:] - along[:, :, :-2]), 0.5 * (across[:, 2:, :] - across[:, :-2, :]))

def global_pad(along_stack, across_stack):
    along = jnp.pad(along_stack, ((0, 0), (0, 0), (1, 1)), mode='wrap')
    across = jnp.pad(across_stack, ((0, 0), (1, 1), (0, 0)))
    return (along, across)

def subcycle(velocity, stresses, statics):
    strength, mass, concentration, drag, push_x, push_y, wet = statics
    along, across = global_pad(velocity, velocity)
    ddx, ddy = slopes(along, across)
    divergence = ddx[0] + ddy[1]
    tension = ddx[0] - ddy[1]
    shearing = ddy[0] + ddx[1]
    delta = jnp.sqrt(divergence * divergence + (tension * tension + shearing * shearing) / ECC_SQUARED + DELTA_FLOOR * DELTA_FLOOR)
    relax = 1.0 / (1.0 + ELASTIC)
    viscous = ELASTIC * strength / delta
    first = wet * (stresses[0] + viscous * (divergence - delta)) * relax
    second = wet * (stresses[1] + viscous * tension / ECC_SQUARED) * relax
    cross = wet * (stresses[2] + viscous * shearing / ECC_SQUARED) * relax
    normal_x = 0.5 * (first + second)
    normal_y = 0.5 * (first - second)
    along_s, across_s = global_pad(jnp.stack([normal_x, cross]), jnp.stack([cross, normal_y]))
    sdx, sdy = slopes(along_s, across_s)
    force_x = sdx[0] + sdy[0]
    force_y = sdx[1] + sdy[1]
    denom = mass + drag + 1.0 - wet
    speed_u = wet * (mass * velocity[0] + force_x + concentration * push_x + CORIOLIS * mass * velocity[1]) / denom
    speed_v = wet * (mass * velocity[1] + force_y + concentration * push_y - CORIOLIS * mass * velocity[0]) / denom
    return (jnp.stack([speed_u, speed_v]), jnp.stack([first, second, cross]))

def reference(thickness, area, ridge_weight, cat_top, land_mask, velocity_u, velocity_v, stress_div, stress_ten, stress_shear, wind_x, wind_y, water_drag):

    def accumulate(level, carry):
        strength, mass, concentration = carry
        height = lax.dynamic_index_in_dim(thickness, level, 0, keepdims=False).astype(jnp.float32)
        present = (level < cat_top).astype(jnp.float32)
        cover = lax.dynamic_index_in_dim(area, level, 0, keepdims=False).astype(jnp.float32) * present
        weight = lax.dynamic_index_in_dim(ridge_weight, level, 0, keepdims=False)
        return (strength + weight * cover * height * height, mass + cover * height, concentration + cover)
    zeros = jnp.zeros(cat_top.shape, jnp.float32)
    strength, mass, concentration = lax.fori_loop(jnp.int32(0), jnp.int32(NCAT), accumulate, (zeros, zeros, zeros))
    wet = land_mask.astype(jnp.float32)
    statics = (strength, mass, concentration, water_drag, wind_x, wind_y, wet)
    velocity = jnp.stack([velocity_u, velocity_v])
    stresses = jnp.stack([stress_div, stress_ten, stress_shear])
    for step in range(SUB):
        velocity, stresses = subcycle(velocity, stresses, statics)
    return (velocity[0], velocity[1], stresses[0], stresses[1], stresses[2])
```

```python
import functools

import jax
import jax.numpy as jnp
from jax import lax
from jax.experimental import pallas as pl
from jax.experimental.pallas import tpu as pltpu
from jax.sharding import PartitionSpec as P

SUB = 4
LANES = 128
EDGE = 8
CHUNK = 32
BLOCK = 16
TOP = 24
MESH = pl.DeviceIdType.MESH

FS, FM, FC, FD, FX, FY, FW, FU, FV, F1, F2, F3 = range(12)
FIELDS = 12


def kernel(
    lat_count,
    lon_count,
    weight,
    thick_hbm,
    area_hbm,
    top_hbm,
    land_hbm,
    u_hbm,
    v_hbm,
    s1_hbm,
    s2_hbm,
    s3_hbm,
    wx_hbm,
    wy_hbm,
    drag_hbm,
    out_u,
    out_v,
    out_1,
    out_2,
    out_3,
    field,
    own,
    other,
    thick,
    area,
    top,
    land,
    pack_left,
    pack_right,
    from_left,
    from_right,
    load_sem,
    x_send,
    x_recv,
    halo_send,
    halo_recv,
    out_sem,
):
    cats, rows, cols = thick.shape
    wide = cols + LANES
    last = cols - LANES
    middle = cols - 2 * LANES
    events = (rows - 2 * BLOCK) // CHUNK
    my_cat = lax.axis_index("cat")
    my_lat = lax.axis_index("lat")
    my_lon = lax.axis_index("lon")
    partner = {"cat": 1 - my_cat}
    west = {"lon": lax.rem(my_lon + lon_count - 1, lon_count)}
    east = {"lon": lax.rem(my_lon + 1, lon_count)}
    north = {"lat": my_lat - 1}
    south = {"lat": my_lat + 1}
    has_north = my_lat > 0
    has_south = my_lat < lat_count - 1

    top_load = pltpu.make_async_copy(top_hbm, top, load_sem.at[0])
    top_load.start()
    strips = ((0, LANES), (last, LANES), (LANES, middle))
    cat_loads = []
    for k, (c0, w) in enumerate(strips):
        pair = (
            pltpu.make_async_copy(
                thick_hbm.at[:, :, pl.ds(c0, w)], thick.at[:, :, pl.ds(c0, w)], load_sem.at[1 + 2 * k]
            ),
            pltpu.make_async_copy(
                area_hbm.at[:, :, pl.ds(c0, w)], area.at[:, :, pl.ds(c0, w)], load_sem.at[2 + 2 * k]
            ),
        )
        for copy in pair:
            copy.start()
        cat_loads.append(pair)
    land_load = pltpu.make_async_copy(land_hbm, land, load_sem.at[7])
    land_load.start()
    field_loads = []
    for k, (f, ref) in enumerate(
        (
            (FU, u_hbm),
            (FV, v_hbm),
            (F1, s1_hbm),
            (F2, s2_hbm),
            (F3, s3_hbm),
            (FX, wx_hbm),
            (FY, wy_hbm),
            (FD, drag_hbm),
        )
    ):
        copy = pltpu.make_async_copy(
            ref, field.at[f, pl.ds(TOP, rows), pl.ds(0, cols)], load_sem.at[8 + k]
        )
        copy.start()
        field_loads.append(copy)

    barrier = pltpu.get_barrier_semaphore()
    for device in (partner, west, east):
        pl.semaphore_signal(barrier, inc=1, device_id=device, device_id_type=MESH)

    @pl.when(has_north)
    def _():
        pl.semaphore_signal(barrier, inc=1, device_id=north, device_id_type=MESH)

    @pl.when(has_south)
    def _():
        pl.semaphore_signal(barrier, inc=1, device_id=south, device_id_type=MESH)

    @pl.when(jnp.logical_not(has_north))
    def _():
        field[:, pl.ds(TOP - EDGE, EDGE), :] = jnp.zeros((FIELDS, EDGE, wide), jnp.float32)

    @pl.when(jnp.logical_not(has_south))
    def _():
        field[:, pl.ds(TOP + rows, EDGE), :] = jnp.zeros((FIELDS, EDGE, wide), jnp.float32)

    base = my_cat * cats

    def partial(r0, count, c0, w):
        def body(i, carry):
            r = pl.multiple_of(r0 + i * BLOCK, BLOCK)
            for c in range(c0, c0 + w, LANES):
                lanes = pl.ds(c, LANES)
                limit = top[pl.ds(r, BLOCK), lanes] - base
                strength = mass = conc = jnp.zeros((BLOCK, LANES), jnp.float32)
                for n in range(cats):
                    height = thick[n, pl.ds(r, BLOCK), lanes].astype(jnp.float32)
                    cover = jnp.where(limit > n, area[n, pl.ds(r, BLOCK), lanes].astype(jnp.float32), 0.0)
                    volume = cover * height
                    conc = conc + cover
                    mass = mass + volume
                    strength = strength + weight[n] * (volume * height)
                own[0, pl.ds(r, BLOCK), lanes] = strength
                own[1, pl.ds(r, BLOCK), lanes] = mass
                own[2, pl.ds(r, BLOCK), lanes] = conc
            return carry

        lax.fori_loop(0, count, body, 0)

    def exchange(slot, r0, height, c0, w):
        part = (pl.ds(0, 3), pl.ds(r0, height), pl.ds(c0, w))
        return pltpu.make_async_remote_copy(
            src_ref=own.at[part],
            dst_ref=other.at[part],
            send_sem=x_send.at[slot],
            recv_sem=x_recv.at[slot],
            device_id=partner,
            device_id_type=MESH,
        )

    def total(r0, count, c0, w):
        def body(i, carry):
            r = pl.multiple_of(r0 + i * BLOCK, BLOCK)
            for f in range(3):
                field[f, pl.ds(pl.multiple_of(r + TOP, 8), BLOCK), pl.ds(c0, w)] = (
                    own[f, pl.ds(r, BLOCK), pl.ds(c0, w)] + other[f, pl.ds(r, BLOCK), pl.ds(c0, w)]
                )
            return carry

        lax.fori_loop(0, count, body, 0)

    border = (
        (0, rows, 0, LANES),
        (0, rows, last, LANES),
        (0, BLOCK, LANES, middle),
        (rows - BLOCK, BLOCK, LANES, middle),
    )
    top_load.wait()
    for slot, (r0, height, c0, w) in enumerate(border):
        if slot < 3:
            for copy in cat_loads[slot]:
                copy.wait()
        partial(r0, height // BLOCK, c0, w)
        if slot == 0:
            pl.semaphore_wait(
                barrier, 3 + has_north.astype(jnp.int32) + has_south.astype(jnp.int32)
            )
        exchange(slot, r0, height, c0, w).start()

    def inner(e):
        return exchange(
            4 + e, pl.multiple_of(BLOCK + e * CHUNK, BLOCK), CHUNK, LANES, middle
        )

    def send_inner(e, carry):
        partial(BLOCK + e * CHUNK, CHUNK // BLOCK, LANES, middle)
        inner(e).start()
        return carry

    lax.fori_loop(0, events, send_inner, 0)

    land_load.wait()

    def wet_body(i, carry):
        r = pl.multiple_of(i * BLOCK, BLOCK)
        field[FW, pl.ds(pl.multiple_of(r + TOP, 8), BLOCK), pl.ds(0, cols)] = land[
            pl.ds(r, BLOCK), :
        ].astype(jnp.float32)
        return carry

    lax.fori_loop(0, rows // BLOCK, wet_body, 0)
    for copy in field_loads:
        copy.wait()

    for slot, (r0, height, c0, w) in enumerate(border):
        exchange(slot, r0, height, c0, w).wait_recv()
        total(r0, height // BLOCK, c0, w)

    def pack_body(i, carry):
        r = pl.multiple_of(i * CHUNK, 8)
        lane = lax.broadcasted_iota(jnp.int32, (CHUNK, LANES), 1)
        source = pl.ds(pl.multiple_of(r + TOP, 8), CHUNK)
        left = field[0, source, pl.ds(0, LANES)]
        right = field[0, source, pl.ds(last, LANES)]
        for f in range(1, FIELDS):
            x = field[f, source, pl.ds(0, LANES)]
            left = jnp.where(lane >= EDGE * f, pltpu.roll(x, EDGE * f, 1), left)
            y = field[f, source, pl.ds(last, LANES)]
            right = jnp.where(lane < LANES - EDGE * f, pltpu.roll(y, LANES - EDGE * f, 1), right)
        pack_left[pl.ds(r, CHUNK), :] = left
        pack_right[pl.ds(r, CHUNK), :] = right
        return carry

    lax.fori_loop(0, rows // CHUNK, pack_body, 0)
    to_east = pltpu.make_async_remote_copy(
        src_ref=pack_right,
        dst_ref=from_left,
        send_sem=halo_send.at[0],
        recv_sem=halo_recv.at[0],
        device_id=east,
        device_id_type=MESH,
    )
    to_west = pltpu.make_async_remote_copy(
        src_ref=pack_left,
        dst_ref=from_right,
        send_sem=halo_send.at[1],
        recv_sem=halo_recv.at[1],
        device_id=west,
        device_id_type=MESH,
    )
    to_east.start()
    to_west.start()
    to_east.wait()
    to_west.wait()

    def unpack_body(i, carry):
        r = pl.multiple_of(i * CHUNK, 8)
        lane = lax.broadcasted_iota(jnp.int32, (CHUNK, LANES), 1)
        x = from_right[pl.ds(r, CHUNK), :]
        y = from_left[pl.ds(r, CHUNK), :]
        for f in range(FIELDS):
            a = pltpu.roll(x, LANES - EDGE * f, 1) if f else x
            b = pltpu.roll(y, EDGE * f, 1) if f else y
            field[f, pl.ds(pl.multiple_of(r + TOP, 8), CHUNK), pl.ds(cols, LANES)] = jnp.where(
                lane < EDGE, a, jnp.where(lane >= LANES - EDGE, b, 0.0)
            )
        return carry

    lax.fori_loop(0, rows // CHUNK, unpack_body, 0)

    def row_copy(source, target, slot, device):
        return pltpu.make_async_remote_copy(
            src_ref=field.at[:, pl.ds(source, EDGE), :],
            dst_ref=field.at[:, pl.ds(target, EDGE), :],
            send_sem=halo_send.at[slot],
            recv_sem=halo_recv.at[slot],
            device_id=device,
            device_id_type=MESH,
        )

    to_north = row_copy(TOP, TOP + rows, 2, north)
    to_south = row_copy(TOP + rows - EDGE, TOP - EDGE, 3, south)

    @pl.when(has_north)
    def _():
        to_north.start()

    @pl.when(has_south)
    def _():
        to_south.start()

    @pl.when(has_north)
    def _():
        to_north.wait_send()
        to_south.wait_recv()

    @pl.when(has_south)
    def _():
        to_south.wait_send()
        to_north.wait_recv()

    third = 1.0 / 3.0

    def derive(i, carry):
        at = pl.ds(pl.multiple_of(BLOCK + i * BLOCK, 8), BLOCK)
        wet = field[FW, at, :]
        mass = field[FM, at, :]
        conc = field[FC, at, :]
        ratio = wet / (mass + field[FD, at, :] + 1.0 - wet)
        force = conc * ratio
        field[FS, at, :] = (2.0 * third) * wet * field[FS, at, :]
        field[FM, at, :] = mass * ratio
        field[FD, at, :] = 0.25 * ratio
        field[FX, at, :] = force * field[FX, at, :]
        field[FY, at, :] = force * field[FY, at, :]
        field[FW, at, :] = third * wet
        return carry

    tall = BLOCK + 2 * EDGE

    def rows_of(x):
        return x[EDGE : EDGE + BLOCK]

    def across(x):
        return rows_of(pltpu.roll(x, tall - 1, 0)) - rows_of(pltpu.roll(x, 1, 0))

    def along(x):
        return pltpu.roll(x, wide - 1, 1) - pltpu.roll(x, 1, 1)

    def stress(i, carry):
        r = BLOCK + i * BLOCK
        around = pl.ds(pl.multiple_of(r - EDGE, 8), tall)
        at = pl.ds(pl.multiple_of(r, 8), BLOCK)
        u = field[FU, around, :]
        v = field[FV, around, :]
        dxu, dyu = along(rows_of(u)), across(u)
        dxv, dyv = along(rows_of(v)), across(v)
        div = dxu + dyv
        ten = dxu - dyv
        shr = dyu + dxv
        inverse = lax.rsqrt(div * div + 0.25 * (ten * ten + shr * shr) + 0.01)
        power = field[FS, at, :]
        keep = field[FW, at, :]
        gain = power * inverse
        quarter = 0.25 * gain
        field[F1, at, :] = keep * field[F1, at, :] + (gain * div - power)
        field[F2, at, :] = keep * field[F2, at, :] + quarter * ten
        field[F3, at, :] = keep * field[F3, at, :] + quarter * shr
        return carry

    def motion(i, carry):
        r = EDGE + i * BLOCK
        around = pl.ds(pl.multiple_of(r - EDGE, 8), tall)
        at = pl.ds(pl.multiple_of(r, 8), BLOCK)
        first = field[F1, around, :]
        second = field[F2, around, :]
        cross = field[F3, around, :]
        total_x = rows_of(first) + rows_of(second)
        total_y = first - second
        bend = across(cross)
        fx = along(total_x) + (bend + bend)
        fy = along(rows_of(cross))
        fy = (fy + fy) + across(total_y)
        u = field[FU, at, :]
        v = field[FV, at, :]
        inertia = field[FM, at, :]
        ratio = field[FD, at, :]
        field[FU, at, :] = inertia * (u + 0.5 * v) + ratio * fx + field[FX, at, :]
        field[FV, at, :] = inertia * (v - 0.5 * u) + ratio * fy + field[FY, at, :]
        return carry

    blocks = (rows + 2 * EDGE) // BLOCK
    per = CHUNK // BLOCK

    def event(e, carry):
        inner(e).wait_recv()
        total(BLOCK + e * CHUNK, CHUNK // BLOCK, LANES, middle)
        first = e == 0
        final = e == events - 1

        def reach(lag, end):
            low = jnp.where(first, 0, 1 + per * e - lag)
            high = jnp.where(final, end, 3 + per * e - lag)
            return low, high

        low, high = reach(0, blocks)
        lax.fori_loop(low, high, derive, 0)

        def cycle(t, inner_carry):
            low, high = reach(t, blocks)
            lax.fori_loop(low, high, stress, 0)
            low, high = reach(t, blocks + 1)
            lax.fori_loop(low, high, motion, 0)
            return inner_carry

        lax.fori_loop(0, SUB, cycle, 0)
        return carry

    lax.fori_loop(0, events, event, 0)

    outs = []
    for k, (f, ref) in enumerate(
        ((FU, out_u), (FV, out_v), (F1, out_1), (F2, out_2), (F3, out_3))
    ):
        copy = pltpu.make_async_copy(
            field.at[f, pl.ds(TOP, rows), pl.ds(0, cols)], ref, out_sem.at[k]
        )
        copy.start()
        outs.append(copy)
    for slot, (r0, height, c0, w) in enumerate(border):
        exchange(slot, r0, height, c0, w).wait_send()

    def drain(e, carry):
        inner(e).wait_send()
        return carry

    lax.fori_loop(0, events, drain, 0)
    for copy in outs:
        copy.wait()


def shards(
    lat_count,
    lon_count,
    thickness,
    area,
    ridge_weight,
    cat_top,
    land_mask,
    velocity_u,
    velocity_v,
    stress_div,
    stress_ten,
    stress_shear,
    wind_x,
    wind_y,
    water_drag,
):
    cats, rows, cols = thickness.shape
    tall = rows + 2 * TOP
    wide = cols + LANES
    f32 = jnp.float32
    events = (rows - 2 * BLOCK) // CHUNK
    anywhere = pl.BlockSpec(memory_space=pl.ANY)
    return pl.pallas_call(
        functools.partial(kernel, lat_count, lon_count),
        out_shape=tuple(jax.ShapeDtypeStruct((rows, cols), f32) for _ in range(5)),
        in_specs=[pl.BlockSpec(memory_space=pltpu.SMEM)] + [anywhere] * 12,
        out_specs=tuple([anywhere] * 5),
        scratch_shapes=[
            pltpu.VMEM((FIELDS, tall, wide), f32),
            pltpu.VMEM((3, rows, cols), f32),
            pltpu.VMEM((3, rows, cols), f32),
            pltpu.VMEM((cats, rows, cols), thickness.dtype),
            pltpu.VMEM((cats, rows, cols), area.dtype),
            pltpu.VMEM((rows, cols), jnp.int32),
            pltpu.VMEM((rows, cols), jnp.int32),
            pltpu.VMEM((rows, LANES), f32),
            pltpu.VMEM((rows, LANES), f32),
            pltpu.VMEM((rows, LANES), f32),
            pltpu.VMEM((rows, LANES), f32),
            pltpu.SemaphoreType.DMA((16,)),
            pltpu.SemaphoreType.DMA((4 + events,)),
            pltpu.SemaphoreType.DMA((4 + events,)),
            pltpu.SemaphoreType.DMA((4,)),
            pltpu.SemaphoreType.DMA((4,)),
            pltpu.SemaphoreType.DMA((5,)),
        ],
        compiler_params=pltpu.CompilerParams(
            collective_id=0, has_side_effects=True, vmem_limit_bytes=56 * 2**20
        ),
        name="ice",
    )(
        ridge_weight,
        thickness,
        area,
        cat_top,
        land_mask,
        velocity_u,
        velocity_v,
        stress_div,
        stress_ten,
        stress_shear,
        wind_x,
        wind_y,
        water_drag,
    )


def solution(mesh):
    body = functools.partial(shards, mesh.shape["lat"], mesh.shape["lon"])
    plane = P("lat", "lon")
    return jax.shard_map(
        body,
        mesh=mesh,
        in_specs=(P("cat", "lat", "lon"), P("cat", "lat", "lon"), P("cat")) + (plane,) * 10,
        out_specs=(plane,) * 5,
        check_vma=False,
    )
```

```python
import functools

import jax
import jax.numpy as jnp
from jax import lax
from jax.experimental import pallas as pl
from jax.experimental.pallas import tpu as pltpu
from jax.sharding import PartitionSpec as P

SUB = 4
LANES = 128
EDGE = 8
CHUNK = 32
BLOCK = 16
TOP = 24
FOLD = 4
MESH = pl.DeviceIdType.MESH

FS, FM, FC, FD, FX, FY, FW, FU, FV, F1, F2, F3 = range(12)
FIELDS = 12


def kernel(
    lat_count,
    lon_count,
    weight,
    thick_hbm,
    area_hbm,
    top_hbm,
    land_hbm,
    u_hbm,
    v_hbm,
    s1_hbm,
    s2_hbm,
    s3_hbm,
    wx_hbm,
    wy_hbm,
    drag_hbm,
    out_u,
    out_v,
    out_1,
    out_2,
    out_3,
    field,
    own,
    other,
    thick,
    area,
    top,
    land,
    pack_left,
    pack_right,
    from_left,
    from_right,
    sum_left,
    sum_right,
    sum_from_left,
    sum_from_right,
    load_sem,
    x_send,
    x_recv,
    halo_send,
    halo_recv,
):
    cats, rows, cols = thick.shape
    wide = cols + LANES
    last = cols - LANES
    middle = cols - 2 * LANES
    events = (rows - 2 * BLOCK) // CHUNK
    my_cat = lax.axis_index("cat")
    my_lat = lax.axis_index("lat")
    my_lon = lax.axis_index("lon")
    partner = {"cat": 1 - my_cat}
    west = {"lon": lax.rem(my_lon + lon_count - 1, lon_count)}
    east = {"lon": lax.rem(my_lon + 1, lon_count)}
    north = {"lat": my_lat - 1}
    south = {"lat": my_lat + 1}
    has_north = my_lat > 0
    has_south = my_lat < lat_count - 1

    top_load = pltpu.make_async_copy(top_hbm, top, load_sem.at[0])
    top_load.start()
    strips = ((0, LANES), (last, LANES), (LANES, middle))
    cat_loads = []
    for k, (c0, w) in enumerate(strips):
        pair = (
            pltpu.make_async_copy(
                thick_hbm.at[:, :, pl.ds(c0, w)], thick.at[:, :, pl.ds(c0, w)], load_sem.at[1 + 2 * k]
            ),
            pltpu.make_async_copy(
                area_hbm.at[:, :, pl.ds(c0, w)], area.at[:, :, pl.ds(c0, w)], load_sem.at[2 + 2 * k]
            ),
        )
        for copy in pair:
            copy.start()
        cat_loads.append(pair)
    land_load = pltpu.make_async_copy(land_hbm, land, load_sem.at[7])
    land_load.start()
    field_loads = []
    for k, (f, ref) in enumerate(
        (
            (FU, u_hbm),
            (FV, v_hbm),
            (F1, s1_hbm),
            (F2, s2_hbm),
            (F3, s3_hbm),
            (FX, wx_hbm),
            (FY, wy_hbm),
            (FD, drag_hbm),
        )
    ):
        copy = pltpu.make_async_copy(
            ref, field.at[f, pl.ds(TOP, rows), pl.ds(0, cols)], load_sem.at[8 + k]
        )
        copy.start()
        field_loads.append(copy)

    barrier = pltpu.get_barrier_semaphore()
    for device in (partner, west, east):
        pl.semaphore_signal(barrier, inc=1, device_id=device, device_id_type=MESH)

    @pl.when(has_north)
    def _():
        pl.semaphore_signal(barrier, inc=1, device_id=north, device_id_type=MESH)

    @pl.when(has_south)
    def _():
        pl.semaphore_signal(barrier, inc=1, device_id=south, device_id_type=MESH)

    @pl.when(jnp.logical_not(has_north))
    def _():
        field[:, pl.ds(TOP - EDGE, EDGE), :] = jnp.zeros((FIELDS, EDGE, wide), jnp.float32)

    @pl.when(jnp.logical_not(has_south))
    def _():
        field[:, pl.ds(TOP + rows, EDGE), :] = jnp.zeros((FIELDS, EDGE, wide), jnp.float32)

    base = my_cat * cats

    def partial(r0, count, c0, w):
        def body(i, carry):
            r = pl.multiple_of(r0 + i * BLOCK, BLOCK)
            for c in range(c0, c0 + w, LANES):
                lanes = pl.ds(c, LANES)
                limit = top[pl.ds(r, BLOCK), lanes] - base
                strength = mass = conc = jnp.zeros((BLOCK, LANES), jnp.float32)
                for n in range(cats):
                    height = thick[n, pl.ds(r, BLOCK), lanes].astype(jnp.float32)
                    cover = jnp.where(limit > n, area[n, pl.ds(r, BLOCK), lanes].astype(jnp.float32), 0.0)
                    volume = cover * height
                    conc = conc + cover
                    mass = mass + volume
                    strength = strength + weight[n] * (volume * height)
                own[0, pl.ds(r, BLOCK), lanes] = strength
                own[1, pl.ds(r, BLOCK), lanes] = mass
                own[2, pl.ds(r, BLOCK), lanes] = conc
            return carry

        lax.fori_loop(0, count, body, 0)

    def exchange(slot, r0, height, c0, w):
        part = (pl.ds(0, 3), pl.ds(r0, height), pl.ds(c0, w))
        return pltpu.make_async_remote_copy(
            src_ref=own.at[part],
            dst_ref=other.at[part],
            send_sem=x_send.at[slot],
            recv_sem=x_recv.at[slot],
            device_id=partner,
            device_id_type=MESH,
        )

    def total(r0, count, c0, w):
        def body(i, carry):
            r = pl.multiple_of(r0 + i * BLOCK, BLOCK)
            for f in range(3):
                field[f, pl.ds(pl.multiple_of(r + TOP, 8), BLOCK), pl.ds(c0, w)] = (
                    own[f, pl.ds(r, BLOCK), pl.ds(c0, w)] + other[f, pl.ds(r, BLOCK), pl.ds(c0, w)]
                )
            return carry

        lax.fori_loop(0, count, body, 0)

    border = (
        (0, rows, 0, LANES),
        (0, rows, last, LANES),
        (0, BLOCK, LANES, middle),
        (rows - BLOCK, BLOCK, LANES, middle),
    )
    top_load.wait()
    for slot, (r0, height, c0, w) in enumerate(border):
        if slot < 3:
            for copy in cat_loads[slot]:
                copy.wait()
        partial(r0, height // BLOCK, c0, w)
        if slot == 0:
            pl.semaphore_wait(
                barrier, 3 + has_north.astype(jnp.int32) + has_south.astype(jnp.int32)
            )
        exchange(slot, r0, height, c0, w).start()

    def inner(e):
        return exchange(
            4 + e, pl.multiple_of(BLOCK + e * CHUNK, BLOCK), CHUNK, LANES, middle
        )

    def send_inner(e, carry):
        partial(BLOCK + e * CHUNK, CHUNK // BLOCK, LANES, middle)
        inner(e).start()
        return carry

    lax.fori_loop(0, events, send_inner, 0)

    land_load.wait()

    def wet_body(i, carry):
        r = pl.multiple_of(i * BLOCK, BLOCK)
        field[FW, pl.ds(pl.multiple_of(r + TOP, 8), BLOCK), pl.ds(0, cols)] = land[
            pl.ds(r, BLOCK), :
        ].astype(jnp.float32)
        return carry

    lax.fori_loop(0, rows // BLOCK, wet_body, 0)
    for copy in field_loads:
        copy.wait()

    def lon_start(entries, buffers, slot):
        left_out, right_out, left_in, right_in = buffers

        def body(i, carry):
            r = pl.multiple_of(i * CHUNK, 8)
            lane = lax.broadcasted_iota(jnp.int32, (CHUNK, LANES), 1)
            left = right = None
            for k, (f, offset) in enumerate(entries):
                source = pl.ds(pl.multiple_of(r + (TOP + offset), 8), CHUNK)
                x = field[f, source, pl.ds(0, LANES)]
                y = field[f, source, pl.ds(last, LANES)]
                if k == 0:
                    left, right = x, y
                else:
                    shift = EDGE * k
                    left = jnp.where(lane >= shift, pltpu.roll(x, shift, 1), left)
                    right = jnp.where(lane < LANES - shift, pltpu.roll(y, LANES - shift, 1), right)
            left_out[pl.ds(r, CHUNK), :] = left
            right_out[pl.ds(r, CHUNK), :] = right
            return carry

        lax.fori_loop(0, left_out.shape[0] // CHUNK, body, 0)
        copies = tuple(
            pltpu.make_async_remote_copy(
                src_ref=source,
                dst_ref=target,
                send_sem=halo_send.at[slot + k],
                recv_sem=halo_recv.at[slot + k],
                device_id=device,
                device_id_type=MESH,
            )
            for k, (source, target, device) in enumerate(
                ((right_out, left_in, east), (left_out, right_in, west))
            )
        )
        for copy in copies:
            copy.start()
        return copies

    def lon_finish(entries, buffers, copies):
        left_in, right_in = buffers[2:]
        for copy in copies:
            copy.wait()

        def body(i, carry):
            r = pl.multiple_of(i * CHUNK, 8)
            lane = lax.broadcasted_iota(jnp.int32, (CHUNK, LANES), 1)
            x = right_in[pl.ds(r, CHUNK), :]
            y = left_in[pl.ds(r, CHUNK), :]
            for k, (f, offset) in enumerate(entries):
                a = pltpu.roll(x, LANES - EDGE * k, 1) if k else x
                b = pltpu.roll(y, EDGE * k, 1) if k else y
                target = pl.ds(pl.multiple_of(r + (TOP + offset), 8), CHUNK)
                field[f, target, pl.ds(cols, LANES)] = jnp.where(
                    lane < EDGE, a, jnp.where(lane >= LANES - EDGE, b, 0.0)
                )
            return carry

        lax.fori_loop(0, left_in.shape[0] // CHUNK, body, 0)

    def lat_start(first, count, slot):
        def row_copy(source, target, at, device):
            return pltpu.make_async_remote_copy(
                src_ref=field.at[pl.ds(first, count), pl.ds(source, EDGE), :],
                dst_ref=field.at[pl.ds(first, count), pl.ds(target, EDGE), :],
                send_sem=halo_send.at[at],
                recv_sem=halo_recv.at[at],
                device_id=device,
                device_id_type=MESH,
            )

        to_north = row_copy(TOP, TOP + rows, slot, north)
        to_south = row_copy(TOP + rows - EDGE, TOP - EDGE, slot + 1, south)

        @pl.when(has_north)
        def _():
            to_north.start()

        @pl.when(has_south)
        def _():
            to_south.start()

        return to_north, to_south

    def lat_finish(to_north, to_south):
        @pl.when(has_north)
        def _():
            to_north.wait_send()
            to_south.wait_recv()

        @pl.when(has_south)
        def _():
            to_south.wait_send()
            to_north.wait_recv()

    wide_pack = (pack_left, pack_right, from_left, from_right)
    input_entries = [(f, 0) for f in range(3, FIELDS)]
    input_copies = lon_start(input_entries, wide_pack, 0)
    lon_finish(input_entries, wide_pack, input_copies)
    input_rows = lat_start(3, FIELDS - 3, 2)
    for slot, (r0, height, c0, w) in enumerate(border):
        exchange(slot, r0, height, c0, w).wait_recv()
        total(r0, height // BLOCK, c0, w)
    short = rows // FOLD
    sum_pack = (sum_left, sum_right, sum_from_left, sum_from_right)
    sum_entries = [(f, g * short) for g in range(FOLD) for f in range(3)]
    sum_copies = lon_start(sum_entries, sum_pack, 4)
    lon_finish(sum_entries, sum_pack, sum_copies)
    sum_rows = lat_start(0, 3, 6)
    lat_finish(*input_rows)
    lat_finish(*sum_rows)

    third = 1.0 / 3.0

    def derive(i, carry):
        at = pl.ds(pl.multiple_of(BLOCK + i * BLOCK, 8), BLOCK)
        wet = field[FW, at, :]
        mass = field[FM, at, :]
        conc = field[FC, at, :]
        ratio = wet / (mass + field[FD, at, :] + 1.0 - wet)
        force = conc * ratio
        field[FS, at, :] = (2.0 * third) * wet * field[FS, at, :]
        field[FM, at, :] = mass * ratio
        field[FD, at, :] = 0.25 * ratio
        field[FX, at, :] = force * field[FX, at, :]
        field[FY, at, :] = force * field[FY, at, :]
        field[FW, at, :] = third * wet
        return carry

    def near(f, r):
        return field.at[f, pl.ds(pl.multiple_of(r - EDGE, 8), BLOCK + 2 * EDGE)]

    def across(read):
        return read(EDGE + 1, EDGE + 1 + BLOCK) - read(EDGE - 1, EDGE - 1 + BLOCK)

    def along(x):
        return pltpu.roll(x, wide - 1, 1) - pltpu.roll(x, 1, 1)

    def stress(i, carry):
        r = pl.multiple_of(BLOCK + i * BLOCK, 8)
        at = pl.ds(r, BLOCK)
        dxu, dyu = along(field[FU, at, :]), across(lambda a, b: near(FU, r)[a:b, :])
        dxv, dyv = along(field[FV, at, :]), across(lambda a, b: near(FV, r)[a:b, :])
        div = dxu + dyv
        ten = dxu - dyv
        shr = dyu + dxv
        inverse = lax.rsqrt(div * div + 0.25 * (ten * ten + shr * shr) + 0.01)
        power = field[FS, at, :]
        keep = field[FW, at, :]
        gain = power * inverse
        quarter = 0.25 * gain
        field[F1, at, :] = keep * field[F1, at, :] + (gain * div - power)
        field[F2, at, :] = keep * field[F2, at, :] + quarter * ten
        field[F3, at, :] = keep * field[F3, at, :] + quarter * shr
        return carry

    def motion(i, carry):
        r = pl.multiple_of(EDGE + i * BLOCK, 8)
        at = pl.ds(r, BLOCK)
        bend = across(lambda a, b: near(F3, r)[a:b, :])
        fx = along(field[F1, at, :] + field[F2, at, :]) + (bend + bend)
        fy = along(field[F3, at, :])
        fy = (fy + fy) + across(lambda a, b: near(F1, r)[a:b, :] - near(F2, r)[a:b, :])
        u = field[FU, at, :]
        v = field[FV, at, :]
        inertia = field[FM, at, :]
        ratio = field[FD, at, :]
        field[FU, at, :] = inertia * (u + 0.5 * v) + ratio * fx + field[FX, at, :]
        field[FV, at, :] = inertia * (v - 0.5 * u) + ratio * fy + field[FY, at, :]
        return carry

    blocks = (rows + 2 * EDGE) // BLOCK
    per = CHUNK // BLOCK

    def event(e, carry):
        inner(e).wait_recv()
        total(BLOCK + e * CHUNK, CHUNK // BLOCK, LANES, middle)
        first = e == 0
        final = e == events - 1

        def reach(lag, end):
            low = jnp.where(first, 0, 1 + per * e - lag)
            high = jnp.where(final, end, 3 + per * e - lag)
            return low, high

        low, high = reach(0, blocks)
        lax.fori_loop(low, high, derive, 0)

        def cycle(t, inner_carry):
            low, high = reach(t, blocks)
            lax.fori_loop(low, high, stress, 0)
            low, high = reach(t, blocks + 1)
            lax.fori_loop(low, high, motion, 0)
            return inner_carry

        lax.fori_loop(0, SUB, cycle, 0)
        return carry

    lax.fori_loop(0, events, event, 0)

    def deliver(i, carry):
        r = pl.multiple_of(i * BLOCK, BLOCK)
        source = pl.ds(pl.multiple_of(r + TOP, 8), BLOCK)
        for f, ref in ((FU, out_u), (FV, out_v), (F1, out_1), (F2, out_2), (F3, out_3)):
            ref[pl.ds(r, BLOCK), :] = field[f, source, pl.ds(0, cols)]
        return carry

    lax.fori_loop(0, rows // BLOCK, deliver, 0)
    for slot, (r0, height, c0, w) in enumerate(border):
        exchange(slot, r0, height, c0, w).wait_send()

    def drain(e, carry):
        inner(e).wait_send()
        return carry

    lax.fori_loop(0, events, drain, 0)


def write_out(*refs):
    sem = refs[10]
    copies = [pltpu.make_async_copy(refs[k], refs[5 + k], sem.at[k]) for k in range(5)]
    for copy in copies:
        copy.start()
    for copy in copies:
        copy.wait()


def shards(
    lat_count,
    lon_count,
    thickness,
    area,
    ridge_weight,
    cat_top,
    land_mask,
    velocity_u,
    velocity_v,
    stress_div,
    stress_ten,
    stress_shear,
    wind_x,
    wind_y,
    water_drag,
):
    cats, rows, cols = thickness.shape
    tall = rows + 2 * TOP
    wide = cols + LANES
    f32 = jnp.float32
    events = (rows - 2 * BLOCK) // CHUNK
    anywhere = pl.BlockSpec(memory_space=pl.ANY)
    results = pl.pallas_call(
        functools.partial(kernel, lat_count, lon_count),
        out_shape=tuple(pltpu.VMEM((rows, cols), f32) for _ in range(5)),
        in_specs=[pl.BlockSpec(memory_space=pltpu.SMEM)] + [anywhere] * 12,
        out_specs=tuple([pl.BlockSpec(memory_space=pltpu.VMEM)] * 5),
        scratch_shapes=[
            pltpu.VMEM((FIELDS, tall, wide), f32),
            pltpu.VMEM((3, rows, cols), f32),
            pltpu.VMEM((3, rows, cols), f32),
            pltpu.VMEM((cats, rows, cols), thickness.dtype),
            pltpu.VMEM((cats, rows, cols), area.dtype),
            pltpu.VMEM((rows, cols), jnp.int32),
            pltpu.VMEM((rows, cols), jnp.int32),
            pltpu.VMEM((rows, LANES), f32),
            pltpu.VMEM((rows, LANES), f32),
            pltpu.VMEM((rows, LANES), f32),
            pltpu.VMEM((rows, LANES), f32),
            pltpu.VMEM((rows // FOLD, LANES), f32),
            pltpu.VMEM((rows // FOLD, LANES), f32),
            pltpu.VMEM((rows // FOLD, LANES), f32),
            pltpu.VMEM((rows // FOLD, LANES), f32),
            pltpu.SemaphoreType.DMA((16,)),
            pltpu.SemaphoreType.DMA((4 + events,)),
            pltpu.SemaphoreType.DMA((4 + events,)),
            pltpu.SemaphoreType.DMA((8,)),
            pltpu.SemaphoreType.DMA((8,)),
        ],
        compiler_params=pltpu.CompilerParams(
            collective_id=0, has_side_effects=True, vmem_limit_bytes=60 * 2**20
        ),
        name="ice",
    )(
        ridge_weight,
        thickness,
        area,
        cat_top,
        land_mask,
        velocity_u,
        velocity_v,
        stress_div,
        stress_ten,
        stress_shear,
        wind_x,
        wind_y,
        water_drag,
    )
    return pl.pallas_call(
        write_out,
        out_shape=tuple(jax.ShapeDtypeStruct((rows, cols), f32) for _ in range(5)),
        in_specs=[pl.BlockSpec(memory_space=pltpu.VMEM)] * 5,
        out_specs=(anywhere,) * 5,
        scratch_shapes=[pltpu.SemaphoreType.DMA((5,))],
        compiler_params=pltpu.CompilerParams(vmem_limit_bytes=4 * 2**20),
        name="write_out",
    )(*results)


def solution(mesh):
    body = functools.partial(shards, mesh.shape["lat"], mesh.shape["lon"])
    plane = P("lat", "lon")
    return jax.shard_map(
        body,
        mesh=mesh,
        in_specs=(P("cat", "lat", "lon"), P("cat", "lat", "lon"), P("cat")) + (plane,) * 10,
        out_specs=(plane,) * 5,
        check_vma=False,
    )
```
